32 devices in a mesh: ctx: 8 (over y, x, core), dp: 4 (over z).
Axes of the slice: x: 2, y: 2, z: 4, core: 2. Of those that a mesh axis runs over, the one named last changes fastest.
Arguments:
- query: bfloat16 [4, 1024, 512], P('dp', 'ctx'), may hold values from -6 to 6
- key_input: bfloat16 [4, 1024, 512], P('dp', 'ctx'), may hold values from -6 to 6
- value_input: bfloat16 [4, 1024, 512], P('dp', 'ctx'), may hold values from -6 to 6
- filter_taps: float32 [1024, 512], P('ctx'), may hold values from -6 to 6
- grad_output: bfloat16 [4, 1024, 512], P('dp', 'ctx'), may hold values from -6 to 6
Outputs:
- output: bfloat16 [4, 1024, 512], P('dp', 'ctx')
- grad_query: bfloat16 [4, 1024, 512], P('dp', 'ctx')
- grad_key: bfloat16 [4, 1024, 512], P('dp', 'ctx')
- grad_value: bfloat16 [4, 1024, 512], P('dp', 'ctx')
- grad_filter: float32 [1024, 512], P('ctx')
The draws below stay inside these ranges and needn't reach their ends.
All inputs are finite; a program needn't handle non-finite values.
Results may differ from the reference program's by a relative error of at most 0.0058.
Values may be sent and summed in bfloat16 or wider, within the bound.
A program may use at most 64 MiB of HBM per device.

```python
import jax
import jax.numpy as jnp
from jax import lax

C = 512
FILTER_LENGTH = 1024
SEQS = 4


def draw_filter_taps(key, part):
    keys = jax.random.split(jax.random.fold_in(key, 71), 4)
    steps = jnp.arange(FILTER_LENGTH, dtype=jnp.float32)
    scales = jnp.exp(jax.random.uniform(keys[0], (C,), jnp.float32, jnp.log(30.0), jnp.log(4.0 * FILTER_LENGTH)))
    noise = jnp.clip(jax.random.normal(keys[1], (FILTER_LENGTH, C), jnp.float32), -6.0, 6.0)
    shard_positions = jax.random.randint(keys[2], (4,), 1, FILTER_LENGTH)
    twiddle_factors = jax.random.uniform(keys[3], (4, C), jnp.float32, 0.5, 0.8)
    log_decay_envelope = -steps[:, None] / scales[None, :]
    for pulse_train in range(4):
        received_block = (jnp.arange(FILTER_LENGTH, dtype=jnp.int32) >= shard_positions[pulse_train]).astype(jnp.float32)
        log_decay_envelope = log_decay_envelope + received_block[:, None] * jnp.log(twiddle_factors[pulse_train])[None, :]
    envelope = jnp.exp(log_decay_envelope)
    norming = 1.0 / jnp.sqrt(jnp.sum(envelope * envelope, axis=0))
    return noise * envelope * norming[None, :]


def levels(stream_key, shape, cuts, least, top_value):
    loudness, own = 1.0, jax.random.fold_in(stream_key, 6)
    for dim, shards_of in cuts:
        draws = jnp.exp(jax.random.uniform(jax.random.fold_in(own, dim), (shards_of,), jnp.float32, least / len(cuts), top_value / len(cuts)))
        loudness = loudness * jnp.repeat(draws, shape[dim] // shards_of).reshape([-1 if axis == dim else 1 for axis in range(len(shape))])
    return loudness


def gaussian(stream_key, shape, deviation, reach, cuts=(), held_as=jnp.bfloat16):
    array = jax.random.normal(stream_key, shape, jnp.float32) * deviation
    if len(cuts) > 0:
        array = levels(stream_key, shape, cuts, -0.22, 0.18) * array
    return jnp.clip(array, min=-reach, max=reach).astype(held_as)


def setup_inputs(seed: int = 0) -> dict:
    key_list = jax.random.split(jax.random.key(seed), 6)
    return {
        "query": gaussian(key_list[0], (SEQS, FILTER_LENGTH, C), 1.0, 6.0, ((0, 4), (1, 8))),
        "key_input": gaussian(key_list[1], (SEQS, FILTER_LENGTH, C), 1.0, 6.0, ((0, 4), (1, 8))),
        "value_input": gaussian(key_list[2], (SEQS, FILTER_LENGTH, C), 1.0, 6.0, ((0, 4), (1, 8))),
        "filter_taps": draw_filter_taps(jax.random.fold_in(key_list[5], 71), 0),
        "grad_output": gaussian(key_list[4], (SEQS, FILTER_LENGTH, C), 1.0, 6.0, ((0, 4), (1, 8))),
    }


def one_sequence(filter_spec, padded, pieces):
    query, key_input, value_input, grad_output = pieces
    length = query.shape[0]
    product = lax.optimization_barrier((key_input.astype(jnp.float32) * value_input.astype(jnp.float32)).astype(jnp.bfloat16))
    grad_mix = lax.optimization_barrier((grad_output.astype(jnp.float32) * query.astype(jnp.float32)).astype(jnp.bfloat16))
    prod_spec = jnp.fft.rfft(product.astype(jnp.float32), n=padded, axis=0)
    mix_spec = jnp.fft.rfft(grad_mix.astype(jnp.float32), n=padded, axis=0)
    mixed = jnp.fft.irfft(filter_spec * prod_spec, n=padded, axis=0)[:length]
    mixed = lax.optimization_barrier(mixed.astype(jnp.bfloat16)).astype(jnp.float32)
    output = (query.astype(jnp.float32) * mixed).astype(jnp.bfloat16)
    grad_query = (grad_output.astype(jnp.float32) * mixed).astype(jnp.bfloat16)
    grad_product = jnp.fft.irfft(mix_spec * jnp.conj(filter_spec), n=padded, axis=0)[:length]
    grad_product = lax.optimization_barrier(grad_product.astype(jnp.bfloat16)).astype(jnp.float32)
    grad_key = (grad_product * value_input.astype(jnp.float32)).astype(jnp.bfloat16)
    grad_value = (grad_product * key_input.astype(jnp.float32)).astype(jnp.bfloat16)
    grad_taps = jnp.fft.irfft(mix_spec * jnp.conj(prod_spec), n=padded, axis=0)[:length].astype(jnp.float32)
    return output, grad_query, grad_key, grad_value, grad_taps


def reference(query, key_input, value_input, filter_taps, grad_output):
    length = query.shape[1]
    padded = 2 * length
    filter_spec = jnp.fft.rfft(filter_taps, n=padded, axis=0)
    results = lax.map(lambda pieces: one_sequence(filter_spec, padded, pieces), (query, key_input, value_input, grad_output))
    output, grad_query, grad_key, grad_value, grad_taps = results
    grad_filter = jnp.sum(grad_taps, axis=0).astype(jnp.float32)
    return output, grad_query, grad_key, grad_value, grad_filter
```

```python
import functools
import math

import jax
import jax.numpy as jnp
import numpy as np
from jax import lax
from jax.experimental import pallas as pl
from jax.experimental.pallas import tpu as pltpu
from jax.sharding import PartitionSpec as P

HIGH = lax.Precision.HIGHEST
MESH = pl.DeviceIdType.MESH
LANES = 128
F32 = jnp.float32
BF16 = jnp.bfloat16


def block_tables(length):
    odd = 2 * np.arange(length, dtype=np.int64)[:, None] + 1
    angle = (odd * np.arange(length, dtype=np.int64)[None, :] % (4 * length)) * (2.0 * math.pi / (4 * length))
    ahead = np.concatenate([np.cos(angle), -np.sin(angle)], axis=0).astype(np.float32)
    back = ahead.T / np.float32(length)

    def split(table):
        high = jnp.asarray(table).astype(BF16)
        low = (jnp.asarray(table) - high.astype(F32)).astype(BF16)
        return high, low

    with jax.ensure_compile_time_eval():
        ahead_high, ahead_low = split(ahead)
        back_high, back_low = split(back)
        return (
            np.asarray(jnp.concatenate([ahead_high, ahead_low], axis=1)),
            np.asarray(jnp.concatenate([back_high, back_low], axis=1)),
        )


def merge(first, second, low):
    half = first.shape[-1] // 2
    turned = pltpu.roll(jnp.where(low, second, first), half, 1)
    return jnp.where(low, first, turned), jnp.where(low, turned, second)


def kernel(
    nctx,
    ndp,
    q_ref,
    k_ref,
    v_ref,
    f_ref,
    g_ref,
    ahead_ref,
    back_ref,
    out_ref,
    gq_ref,
    gk_ref,
    gv_ref,
    gf_ref,
    send1,
    rx1,
    sig,
    wei,
    oth,
    gfs,
    rs_send,
    rs_rx,
    g2_send,
    g2_rx,
    mg_send,
    mg_rx,
    s1_send,
    s1_recv,
    rs_ssem,
    rs_rsem,
    g2_ssem,
    g2_rsem,
    mg_ssem,
    mg_rsem,
):
    me = lax.axis_index("ctx")
    row = lax.axis_index("dp")
    length = q_ref.shape[1]
    hl = length // 2
    tiles = nctx // 2

    barrier = pltpu.get_barrier_semaphore()
    for oc in range(nctx):
        for od in range(ndp):
            if oc or od:
                pl.semaphore_signal(
                    barrier,
                    inc=1,
                    device_id={"ctx": lax.rem(me + oc, nctx), "dp": lax.rem(row + od, ndp)},
                    device_id_type=MESH,
                )

    low = lax.broadcasted_iota(jnp.int32, (length, LANES), 1) < LANES // 2
    low_h = lax.broadcasted_iota(jnp.int32, (hl, LANES), 1) < LANES // 2
    for p in range(tiles):
        cols = slice(p * LANES, (p + 1) * LANES)
        x = (k_ref[0, :, cols].astype(F32) * v_ref[0, :, cols].astype(F32)).astype(BF16).astype(F32)
        g = (g_ref[0, :, cols].astype(F32) * q_ref[0, :, cols].astype(F32)).astype(BF16).astype(F32)
        even, odd = merge(x, g, low)
        send1[2 * p, 0:length, :] = even.astype(BF16)
        send1[2 * p + 1, 0:length, :] = odd.astype(BF16)
        even, odd = merge(f_ref[0:hl, cols], f_ref[hl:length, cols], low_h)
        send1[2 * p, length : length + hl, :] = even.astype(BF16)
        send1[2 * p + 1, length : length + hl, :] = odd.astype(BF16)

    pl.semaphore_wait(barrier, nctx * ndp - 1)

    def copy1(peer, slot):
        return pltpu.make_async_remote_copy(
            src_ref=send1.at[peer],
            dst_ref=rx1.at[slot],
            send_sem=s1_send.at[peer],
            recv_sem=s1_recv.at[slot],
            device_id={"ctx": peer, "dp": row},
            device_id_type=MESH,
        )

    order = [nctx // 2 + o for o in range(nctx // 2)] + list(range(1, nctx // 2))
    peers = [lax.rem(me + o, nctx) for o in order]
    for peer in peers:
        copy1(peer, me).start()
    rx1[pl.ds(me, 1)] = send1[pl.ds(me, 1)]

    def transform(src):
        z = rx1[src, 0:length, :]
        fa = rx1[src, length : length + hl, :].astype(F32)
        turned = pltpu.roll(fa, LANES // 2, 1)
        w = jnp.concatenate([jnp.where(low_h, fa, turned), jnp.where(low_h, turned, fa)], axis=0).astype(BF16)
        both = jnp.concatenate([z, w], axis=1)
        spec = jnp.dot(ahead_ref[...], jnp.concatenate([both, both], axis=0), preferred_element_type=F32)
        sig[src] = spec[:, 0:LANES]
        wei[src] = spec[:, LANES:]

    transform(me)
    for peer in reversed(peers):
        copy1(peer, peer).wait_recv()
        transform(peer)

    lane8 = lax.broadcasted_iota(jnp.int32, (8, LANES), 1) < LANES // 2
    parity = lax.rem(lax.broadcasted_iota(jnp.int32, (8, LANES), 0), 2)
    alt = jnp.where(parity == 0, 1.0, -1.0).astype(F32)
    lane_sign = jnp.where(lane8, 1.0, -1.0).astype(F32)
    both_sign = alt * lane_sign

    @pl.loop(0, length // 8)
    def _(i):
        re = pl.ds(pl.multiple_of(i * 8, 8), 8)
        im = pl.ds(pl.multiple_of(length + i * 8, 8), 8)
        s_re = [sig[d, re, :] for d in range(nctx)]
        s_im = [sig[d, im, :] for d in range(nctx)]
        u_re = [jnp.where(lane8, pltpu.roll(a, LANES // 2, 1), a) for a in s_re]
        u_im = [jnp.where(lane8, pltpu.roll(a, LANES // 2, 1), a) for a in s_im]
        x_re = [s_re[0]] + [s_re[n] - alt * s_im[n - 1] for n in range(1, nctx)]
        x_im = [s_im[0]] + [s_im[n] + alt * s_re[n - 1] for n in range(1, nctx)]
        v_re = [jnp.where(lane8, x_re[n], 0.0) for n in range(tiles)]
        v_im = [jnp.where(lane8, x_im[n], 0.0) for n in range(tiles)]
        for n in range(tiles, nctx):
            v_re.append(jnp.where(lane8, x_re[n], pltpu.roll(x_re[n - tiles], LANES // 2, 1)))
            v_im.append(jnp.where(lane8, x_im[n], pltpu.roll(x_im[n - tiles], LANES // 2, 1)))
        for j in range(tiles):
            a_re = jnp.zeros((8, LANES), F32)
            a_im = jnp.zeros((8, LANES), F32)
            for m in range(j, nctx):
                n = m - j
                a_re = a_re + u_re[m] * v_re[n] + u_im[m] * v_im[n]
                a_im = a_im + u_im[m] * v_re[n] - u_re[m] * v_im[n]
            gfs[j, re, :] = a_re
            gfs[j, im, :] = a_im

    def inverse(spec):
        high = spec.astype(BF16)
        return jnp.dot(back_ref[...], jnp.concatenate([high, high], axis=0), preferred_element_type=F32)

    def copy_rs(peer, slot):
        return pltpu.make_async_remote_copy(
            src_ref=rs_send.at[peer],
            dst_ref=rs_rx.at[slot],
            send_sem=rs_ssem.at[peer],
            recv_sem=rs_rsem.at[slot],
            device_id={"ctx": me, "dp": peer},
            device_id_type=MESH,
        )

    for j in range(tiles):
        rs_send[j] = inverse(gfs[j]).astype(BF16)
    rows_peers = [lax.rem(row + o, ndp) for o in range(1, ndp)]
    for peer in rows_peers:
        copy_rs(peer, row).start()

    @pl.loop(0, length // 8)
    def _(i):
        re = pl.ds(pl.multiple_of(i * 8, 8), 8)
        im = pl.ds(pl.multiple_of(length + i * 8, 8), 8)
        s_re = [sig[d, re, :] for d in range(nctx)]
        s_im = [sig[d, im, :] for d in range(nctx)]
        q_re = [jnp.where(lane8, s_re[n], s_re[nctx - 1 - n]) for n in range(nctx)]
        q_im = [jnp.where(lane8, s_im[n], s_im[nctx - 1 - n]) for n in range(nctx)]
        z_re = [q_re[0]] + [q_re[n] - both_sign * q_im[n - 1] for n in range(1, nctx)]
        z_im = [q_im[0]] + [q_im[n] + both_sign * q_re[n - 1] for n in range(1, nctx)]
        w_re = [wei[d, re, :] for d in range(nctx)]
        w_im = [wei[d, im, :] * lane_sign for d in range(nctx)]
        o_re, o_im = [], []
        for n in range(nctx):
            a_re = jnp.zeros((8, LANES), F32)
            a_im = jnp.zeros((8, LANES), F32)
            for j in range(n + 1):
                a_re = a_re + w_re[j] * z_re[n - j] - w_im[j] * z_im[n - j]
                a_im = a_im + w_re[j] * z_im[n - j] + w_im[j] * z_re[n - j]
            o_re.append(a_re)
            o_im.append(a_im)
        for d in range(nctx):
            oth[d, re, :] = jnp.where(lane8, o_re[d], o_re[nctx - 1 - d])
            oth[d, im, :] = jnp.where(lane8, o_im[d], o_im[nctx - 1 - d])

    def copy_mg(peer, slot):
        return pltpu.make_async_remote_copy(
            src_ref=mg_send.at[peer],
            dst_ref=mg_rx.at[slot],
            send_sem=mg_ssem.at[peer],
            recv_sem=mg_rsem.at[slot],
            device_id={"ctx": peer, "dp": row},
            device_id_type=MESH,
        )

    for at, peer in enumerate(peers):
        mg_send[peer] = inverse(oth[peer]).astype(BF16)
        if at:
            copy_mg(peers[at - 1], me).start()
    mg_rx[me] = inverse(oth[me]).astype(BF16)
    copy_mg(peers[-1], me).start()

    total = rs_send[row].astype(F32)
    for peer in rows_peers:
        copy_rs(peer, peer).wait_recv()
        total = total + rs_rx[peer].astype(F32)
    first, second = merge(total[0:hl], total[hl:length], low_h)
    g2_send[0] = first.astype(BF16)
    g2_send[1] = second.astype(BF16)

    def copy_g2(part, to_row, slot):
        return pltpu.make_async_remote_copy(
            src_ref=g2_send.at[part],
            dst_ref=g2_rx.at[slot],
            send_sem=g2_ssem.at[part, to_row],
            recv_sem=g2_rsem.at[slot],
            device_id={"ctx": row + part * tiles, "dp": to_row},
            device_id_type=MESH,
        )

    for part in range(2):
        for o in range(1, ndp):
            copy_g2(part, lax.rem(row + o, ndp), me).start()
        mine = me == row + part * tiles

        @pl.when(mine)
        def _():
            g2_rx[me] = g2_send[part]

        @pl.when(jnp.logical_not(mine))
        def _():
            copy_g2(part, row, me).start()

    for peer in peers:
        copy_mg(peer, peer).wait_recv()
    for p in range(tiles):
        cols = slice(p * LANES, (p + 1) * LANES)
        mixed, back = merge(mg_rx[2 * p].astype(F32), mg_rx[2 * p + 1].astype(F32), low)
        out_ref[0, :, cols] = (q_ref[0, :, cols].astype(F32) * mixed).astype(BF16)
        gq_ref[0, :, cols] = (g_ref[0, :, cols].astype(F32) * mixed).astype(BF16)
        gk_ref[0, :, cols] = (v_ref[0, :, cols].astype(F32) * back).astype(BF16)
        gv_ref[0, :, cols] = (k_ref[0, :, cols].astype(F32) * back).astype(BF16)

    from_row = lax.rem(me, tiles)
    for c in range(nctx):
        outside = jnp.logical_not(jnp.logical_and(me == c, row == from_row))

        @pl.when(outside)
        def _():
            copy_g2(0, row, c).wait_recv()

    for p in range(tiles):
        cols = slice(p * LANES, (p + 1) * LANES)
        top, bottom = merge(g2_rx[2 * p].astype(F32), g2_rx[2 * p + 1].astype(F32), low_h)
        gf_ref[0:hl, cols] = top
        gf_ref[hl:length, cols] = bottom

    for peer in peers:
        copy1(peer, me).wait_send()
        copy_mg(peer, me).wait_send()
    for peer in rows_peers:
        copy_rs(peer, row).wait_send()
    for part in range(2):
        for o in range(1, ndp):
            copy_g2(part, lax.rem(row + o, ndp), me).wait_send()

        @pl.when(jnp.logical_not(me == row + part * tiles))
        def _():
            copy_g2(part, row, me).wait_send()


def fused(nctx, ndp, query, key_input, value_input, filter_taps, grad_output):
    length, channels = query.shape[1], query.shape[2]
    ahead, back = block_tables(length)
    vm = pl.BlockSpec(memory_space=pltpu.VMEM)
    wide = jax.ShapeDtypeStruct(query.shape, BF16)
    hl, tiles = length // 2, nctx // 2
    dma = pltpu.SemaphoreType.DMA
    return pl.pallas_call(
        functools.partial(kernel, nctx, ndp),
        out_shape=(wide, wide, wide, wide, jax.ShapeDtypeStruct((length, channels), F32)),
        in_specs=[vm] * 7,
        out_specs=(vm,) * 5,
        scratch_shapes=[
            pltpu.VMEM((nctx, length + hl, LANES), BF16),
            pltpu.VMEM((nctx, length + hl, LANES), BF16),
            pltpu.VMEM((nctx, 2 * length, LANES), F32),
            pltpu.VMEM((nctx, 2 * length, LANES), F32),
            pltpu.VMEM((nctx, 2 * length, LANES), F32),
            pltpu.VMEM((tiles, 2 * length, LANES), F32),
            pltpu.VMEM((tiles, length, LANES), BF16),
            pltpu.VMEM((ndp, length, LANES), BF16),
            pltpu.VMEM((2, hl, LANES), BF16),
            pltpu.VMEM((nctx, hl, LANES), BF16),
            pltpu.VMEM((nctx, length, LANES), BF16),
            pltpu.VMEM((nctx, length, LANES), BF16),
            dma((nctx,)),
            dma((nctx,)),
            dma((ndp,)),
            dma((ndp,)),
            dma((2, ndp)),
            dma((nctx,)),
            dma((nctx,)),
            dma((nctx,)),
        ],
        compiler_params=pltpu.CompilerParams(collective_id=0, has_side_effects=True),
    )(query, key_input, value_input, filter_taps, grad_output, jnp.asarray(ahead), jnp.asarray(back))


def build_tables(length):
    padded = 2 * length
    columns = 1
    while columns * columns < padded and length % (2 * columns) == 0:
        columns = columns * 2
    row_count = padded // columns
    col_index = jnp.arange(columns, dtype=jnp.int32)
    row_index = jnp.arange(row_count, dtype=jnp.int32)
    col_angle = (col_index[:, None] * col_index[None, :] % columns).astype(jnp.float32) * (
        2.0 * math.pi / columns
    )
    row_angle = (row_index[:, None] * row_index[None, :] % row_count).astype(jnp.float32) * (
        2.0 * math.pi / row_count
    )
    twist_angle = (row_index[:, None] * col_index[None, :] % padded).astype(jnp.float32) * (
        2.0 * math.pi / padded
    )
    return (
        jnp.cos(col_angle),
        -jnp.sin(col_angle),
        jnp.cos(row_angle),
        -jnp.sin(row_angle),
        jnp.cos(twist_angle),
        -jnp.sin(twist_angle),
        row_count,
        columns,
        padded,
    )


def forward(signal, tables):
    col_real, col_imag, row_real, row_imag, twist_real, twist_imag, row_count, columns, padded = (
        tables
    )
    half_rows = row_count // 2
    blocks = signal.reshape(signal.shape[0], half_rows, columns, signal.shape[2])
    section_real = jnp.einsum("kn,snac->scka", row_real[:, :half_rows], blocks, precision=HIGH)
    section_imag = jnp.einsum("kn,snac->scka", row_imag[:, :half_rows], blocks, precision=HIGH)
    turned_real = section_real * twist_real - section_imag * twist_imag
    turned_imag = section_real * twist_imag + section_imag * twist_real
    spec_real = jnp.einsum("scka,aj->sckj", turned_real, col_real, precision=HIGH) - jnp.einsum(
        "scka,aj->sckj", turned_imag, col_imag, precision=HIGH
    )
    spec_imag = jnp.einsum("scka,aj->sckj", turned_real, col_imag, precision=HIGH) + jnp.einsum(
        "scka,aj->sckj", turned_imag, col_real, precision=HIGH
    )
    return (spec_real, spec_imag)


def inverse(spec, tables):
    col_real, col_imag, row_real, row_imag, twist_real, twist_imag, row_count, columns, padded = (
        tables
    )
    spec_real, spec_imag = spec
    half_rows = row_count // 2
    section_real = jnp.einsum("scka,aj->sckj", spec_real, col_real, precision=HIGH) + jnp.einsum(
        "scka,aj->sckj", spec_imag, col_imag, precision=HIGH
    )
    section_imag = jnp.einsum("scka,aj->sckj", spec_imag, col_real, precision=HIGH) - jnp.einsum(
        "scka,aj->sckj", spec_real, col_imag, precision=HIGH
    )
    turned_real = section_real * twist_real + section_imag * twist_imag
    turned_imag = section_imag * twist_real - section_real * twist_imag
    signal = jnp.einsum(
        "nk,scka->snac", row_real[:half_rows], turned_real, precision=HIGH
    ) + jnp.einsum("nk,scka->snac", row_imag[:half_rows], turned_imag, precision=HIGH)
    return signal.reshape(signal.shape[0], half_rows * columns, signal.shape[3]) * (1.0 / padded)


def times_spec(first, second):
    return (
        first[0] * second[0] - first[1] * second[1],
        first[0] * second[1] + first[1] * second[0],
    )


def times_conj(first, second):
    return (
        first[0] * second[0] + first[1] * second[1],
        first[1] * second[0] - first[0] * second[1],
    )


def local(query, key_input, value_input, filter_taps, grad_output):
    product = (key_input.astype(jnp.float32) * value_input.astype(jnp.float32)).astype(jnp.bfloat16)
    grad_mix = (grad_output.astype(jnp.float32) * query.astype(jnp.float32)).astype(jnp.bfloat16)
    owned_filter = lax.all_to_all(filter_taps, "ctx", split_axis=1, concat_axis=0, tiled=True)
    tables = build_tables(owned_filter.shape[0])
    filter_spec = forward(owned_filter[None], tables)
    local_product = lax.all_to_all(product, "ctx", split_axis=2, concat_axis=1, tiled=True)
    prod_spec = forward(local_product.astype(jnp.float32), tables)
    owned_mixed = inverse(times_spec(filter_spec, prod_spec), tables).astype(jnp.bfloat16)
    owned_mixed, prod_spec = (owned_mixed, prod_spec)
    mixed = lax.all_to_all(owned_mixed, "ctx", split_axis=1, concat_axis=2, tiled=True)
    owned_grad = lax.all_to_all(grad_mix, "ctx", split_axis=2, concat_axis=1, tiled=True)
    grad_spec = forward(owned_grad.astype(jnp.float32), tables)
    owned_back = inverse(times_conj(grad_spec, filter_spec), tables).astype(jnp.bfloat16)
    taps_spec = times_conj(grad_spec, prod_spec)
    owned_back, taps_spec = (
        owned_back,
        (jnp.sum(taps_spec[0], axis=0), jnp.sum(taps_spec[1], axis=0)),
    )
    grad_product = lax.all_to_all(owned_back, "ctx", split_axis=1, concat_axis=2, tiled=True)
    mixed_wide = mixed.astype(jnp.float32)
    back_wide = grad_product.astype(jnp.float32)
    output = (query.astype(jnp.float32) * mixed_wide).astype(jnp.bfloat16)
    grad_query = (grad_output.astype(jnp.float32) * mixed_wide).astype(jnp.bfloat16)
    grad_key = (back_wide * value_input.astype(jnp.float32)).astype(jnp.bfloat16)
    grad_value = (back_wide * key_input.astype(jnp.float32)).astype(jnp.bfloat16)
    local_taps = inverse((taps_spec[0][None], taps_spec[1][None]), tables)[0]
    owned_taps = lax.psum(local_taps, "dp")
    grad_filter = lax.all_to_all(owned_taps, "ctx", split_axis=0, concat_axis=1, tiled=True)
    return (output, grad_query, grad_key, grad_value, grad_filter)


def plan(mesh, query, key_input, value_input, filter_taps, grad_output):
    nctx, ndp = mesh.shape["ctx"], mesh.shape["dp"]
    sequences, length, channels = query.shape
    fits = 2 * channels == nctx * LANES and nctx == 2 * ndp and sequences == 1 and length % 32 == 0 and length <= LANES
    run = functools.partial(fused, nctx, ndp) if fits else local
    return run(query, key_input, value_input, filter_taps, grad_output)


def solution(mesh):
    wide, taps = P("dp", "ctx", None), P("ctx", None)
    return jax.shard_map(
        functools.partial(plan, mesh),
        mesh=mesh,
        in_specs=(wide, wide, wide, taps, wide),
        out_specs=(wide, wide, wide, wide, taps),
        check_vma=False,
    )
```

```python
import functools
import math

import jax
import jax.numpy as jnp
import numpy as np
from jax import lax
from jax.experimental import pallas as pl
from jax.experimental.pallas import tpu as pltpu
from jax.sharding import PartitionSpec as P

HIGH = lax.Precision.HIGHEST
MESH = pl.DeviceIdType.MESH
LANES = 128
VMEM_BYTES = 67043328
F32 = jnp.float32
BF16 = jnp.bfloat16


def block_tables(length):
    odd = 2 * np.arange(length, dtype=np.int64)[:, None] + 1
    angle = (odd * np.arange(length, dtype=np.int64)[None, :] % (4 * length)) * (2.0 * math.pi / (4 * length))
    ahead = np.concatenate([np.cos(angle), -np.sin(angle)], axis=0).astype(np.float32)
    back = ahead.T / np.float32(length)

    def split(table):
        high = jnp.asarray(table).astype(BF16)
        low = (jnp.asarray(table) - high.astype(F32)).astype(BF16)
        return high, low

    with jax.ensure_compile_time_eval():
        ahead_high, ahead_low = split(ahead)
        back_high, back_low = split(back)
        return (
            np.asarray(jnp.concatenate([ahead_high, ahead_low], axis=1)),
            np.asarray(jnp.concatenate([back_high, back_low], axis=1)),
        )


def merge(first, second, low):
    half = first.shape[-1] // 2
    turned = pltpu.roll(jnp.where(low, second, first), half, 1)
    return jnp.where(low, first, turned), jnp.where(low, turned, second)


def kernel(
    nctx,
    ndp,
    q_hbm,
    k_hbm,
    v_hbm,
    f_hbm,
    g_hbm,
    ahead_hbm,
    back_hbm,
    mg_rx,
    g2_rx,
    qv,
    kv,
    vv,
    gv,
    fv,
    ahead_v,
    back_v,
    send1,
    rx1,
    sendf,
    rxf,
    sig,
    wei,
    oth,
    gfs,
    rs_send,
    rs_rx,
    g2_send,
    mg_send,
    load_sem,
    s1_send,
    s1_recv,
    sf_send,
    sf_recv,
    rs_ssem,
    rs_rsem,
    g2_ssem,
    g2_rsem,
    mg_ssem,
    mg_rsem,
):
    me = lax.axis_index("ctx")
    row = lax.axis_index("dp")
    length = qv.shape[1]
    hl = length // 2
    tiles = nctx // 2

    pairs = ((k_hbm, kv), (v_hbm, vv), (g_hbm, gv), (q_hbm, qv), (f_hbm, fv), (ahead_hbm, ahead_v), (back_hbm, back_v))
    loads = [pltpu.make_async_copy(src, dst, load_sem.at[n]) for n, (src, dst) in enumerate(pairs)]
    for load in loads:
        load.start()

    barrier = pltpu.get_barrier_semaphore()
    for oc in range(nctx):
        for od in range(ndp):
            if (oc == 0) != (od == 0):
                pl.semaphore_signal(
                    barrier,
                    inc=1,
                    device_id={"ctx": lax.rem(me + oc, nctx), "dp": lax.rem(row + od, ndp)},
                    device_id_type=MESH,
                )

    low = lax.broadcasted_iota(jnp.int32, (length, LANES), 1) < LANES // 2
    low_h = lax.broadcasted_iota(jnp.int32, (hl, LANES), 1) < LANES // 2
    for load in loads[:4]:
        load.wait()
    for p in range(tiles):
        cols = slice(p * LANES, (p + 1) * LANES)
        x = (kv[0, :, cols].astype(F32) * vv[0, :, cols].astype(F32)).astype(BF16).astype(F32)
        g = (gv[0, :, cols].astype(F32) * qv[0, :, cols].astype(F32)).astype(BF16).astype(F32)
        even, odd = merge(x, g, low)
        send1[2 * p] = even.astype(BF16)
        send1[2 * p + 1] = odd.astype(BF16)

    pl.semaphore_wait(barrier, nctx + ndp - 2)

    def copy1(peer, slot):
        return pltpu.make_async_remote_copy(
            src_ref=send1.at[peer],
            dst_ref=rx1.at[slot],
            send_sem=s1_send.at[peer],
            recv_sem=s1_recv.at[slot],
            device_id={"ctx": peer, "dp": row},
            device_id_type=MESH,
        )

    def copyf(peer, slot):
        return pltpu.make_async_remote_copy(
            src_ref=sendf.at[peer],
            dst_ref=rxf.at[slot],
            send_sem=sf_send.at[peer],
            recv_sem=sf_recv.at[slot],
            device_id={"ctx": peer, "dp": row},
            device_id_type=MESH,
        )

    order = [nctx // 2 + o for o in range(nctx // 2)] + list(range(1, nctx // 2))
    peers = [lax.rem(me + o, nctx) for o in order]
    for peer in peers:
        copy1(peer, me).start()
    loads[4].wait()
    for p in range(tiles):
        cols = slice(p * LANES, (p + 1) * LANES)
        even, odd = merge(fv[0:hl, cols], fv[hl:length, cols], low_h)
        sendf[2 * p] = even.astype(BF16)
        sendf[2 * p + 1] = odd.astype(BF16)
    for load in loads[5:]:
        load.wait()
    for peer in peers:
        copyf(peer, me).start()

    def transform(z):
        return jnp.dot(ahead_v[...], jnp.concatenate([z, z], axis=0), preferred_element_type=F32)

    def weigh(fa):
        fa = fa.astype(F32)
        turned = pltpu.roll(fa, LANES // 2, 1)
        w = jnp.concatenate([jnp.where(low_h, fa, turned), jnp.where(low_h, turned, fa)], axis=0)
        return transform(w.astype(BF16))

    sig[me] = transform(send1[me])
    for peer in reversed(peers):
        copy1(peer, peer).wait_recv()
        sig[peer] = transform(rx1[peer])

    lane8 = lax.broadcasted_iota(jnp.int32, (8, LANES), 1) < LANES // 2
    parity = lax.rem(lax.broadcasted_iota(jnp.int32, (8, LANES), 0), 2)
    alt = jnp.where(parity == 0, 1.0, -1.0).astype(F32)
    lane_sign = jnp.where(lane8, 1.0, -1.0).astype(F32)
    both_sign = alt * lane_sign

    @pl.loop(0, length // 8)
    def _(i):
        re = pl.ds(pl.multiple_of(i * 8, 8), 8)
        im = pl.ds(pl.multiple_of(length + i * 8, 8), 8)
        s_re = [sig[d, re, :] for d in range(nctx)]
        s_im = [sig[d, im, :] for d in range(nctx)]
        u_re = [jnp.where(lane8, pltpu.roll(a, LANES // 2, 1), a) for a in s_re]
        u_im = [jnp.where(lane8, pltpu.roll(a, LANES // 2, 1), a) for a in s_im]
        x_re = [s_re[0]] + [s_re[n] - alt * s_im[n - 1] for n in range(1, nctx)]
        x_im = [s_im[0]] + [s_im[n] + alt * s_re[n - 1] for n in range(1, nctx)]
        v_re = [jnp.where(lane8, x_re[n], 0.0) for n in range(tiles)]
        v_im = [jnp.where(lane8, x_im[n], 0.0) for n in range(tiles)]
        for n in range(tiles, nctx):
            v_re.append(jnp.where(lane8, x_re[n], pltpu.roll(x_re[n - tiles], LANES // 2, 1)))
            v_im.append(jnp.where(lane8, x_im[n], pltpu.roll(x_im[n - tiles], LANES // 2, 1)))
        for j in range(tiles):
            a_re = jnp.zeros((8, LANES), F32)
            a_im = jnp.zeros((8, LANES), F32)
            for m in range(j, nctx):
                n = m - j
                a_re = a_re + u_re[m] * v_re[n] + u_im[m] * v_im[n]
                a_im = a_im + u_im[m] * v_re[n] - u_re[m] * v_im[n]
            gfs[j, re, :] = a_re
            gfs[j, im, :] = a_im

    def inverse(spec):
        high = spec.astype(BF16)
        return jnp.dot(back_v[...], jnp.concatenate([high, high], axis=0), preferred_element_type=F32)

    def copy_rs(peer, slot):
        return pltpu.make_async_remote_copy(
            src_ref=rs_send.at[peer],
            dst_ref=rs_rx.at[slot],
            send_sem=rs_ssem.at[peer],
            recv_sem=rs_rsem.at[slot],
            device_id={"ctx": me, "dp": peer},
            device_id_type=MESH,
        )

    for j in range(tiles):
        rs_send[j] = inverse(gfs[j]).astype(BF16)
    rows_peers = [lax.rem(row + o, ndp) for o in range(1, ndp)]
    for peer in rows_peers:
        copy_rs(peer, row).start()

    wei[me] = weigh(sendf[me])
    for peer in reversed(peers):
        copyf(peer, peer).wait_recv()
        wei[peer] = weigh(rxf[peer])

    @pl.loop(0, length // 8)
    def _(i):
        re = pl.ds(pl.multiple_of(i * 8, 8), 8)
        im = pl.ds(pl.multiple_of(length + i * 8, 8), 8)
        s_re = [sig[d, re, :] for d in range(nctx)]
        s_im = [sig[d, im, :] for d in range(nctx)]
        q_re = [jnp.where(lane8, s_re[n], s_re[nctx - 1 - n]) for n in range(nctx)]
        q_im = [jnp.where(lane8, s_im[n], s_im[nctx - 1 - n]) for n in range(nctx)]
        z_re = [q_re[0]] + [q_re[n] - both_sign * q_im[n - 1] for n in range(1, nctx)]
        z_im = [q_im[0]] + [q_im[n] + both_sign * q_re[n - 1] for n in range(1, nctx)]
        w_re = [wei[d, re, :] for d in range(nctx)]
        w_im = [wei[d, im, :] * lane_sign for d in range(nctx)]
        o_re, o_im = [], []
        for n in range(nctx):
            a_re = jnp.zeros((8, LANES), F32)
            a_im = jnp.zeros((8, LANES), F32)
            for j in range(n + 1):
                a_re = a_re + w_re[j] * z_re[n - j] - w_im[j] * z_im[n - j]
                a_im = a_im + w_re[j] * z_im[n - j] + w_im[j] * z_re[n - j]
            o_re.append(a_re)
            o_im.append(a_im)
        for d in range(nctx):
            oth[d, re, :] = jnp.where(lane8, o_re[d], o_re[nctx - 1 - d])
            oth[d, im, :] = jnp.where(lane8, o_im[d], o_im[nctx - 1 - d])

    def copy_mg(peer, slot):
        return pltpu.make_async_remote_copy(
            src_ref=mg_send.at[peer],
            dst_ref=mg_rx.at[slot],
            send_sem=mg_ssem.at[peer],
            recv_sem=mg_rsem.at[slot],
            device_id={"ctx": peer, "dp": row},
            device_id_type=MESH,
        )

    for at, peer in enumerate(peers):
        mg_send[peer] = inverse(oth[peer]).astype(BF16)
        if at:
            copy_mg(peers[at - 1], me).start()
    mg_rx[me] = inverse(oth[me]).astype(BF16)
    copy_mg(peers[-1], me).start()

    total = rs_send[row].astype(F32)
    for peer in rows_peers:
        copy_rs(peer, peer).wait_recv()
        total = total + rs_rx[peer].astype(F32)
    first, second = merge(total[0:hl], total[hl:length], low_h)
    g2_send[0] = first.astype(BF16)
    g2_send[1] = second.astype(BF16)

    def copy_g2(part, to_row, slot):
        return pltpu.make_async_remote_copy(
            src_ref=g2_send.at[part],
            dst_ref=g2_rx.at[slot],
            send_sem=g2_ssem.at[part, to_row],
            recv_sem=g2_rsem.at[slot],
            device_id={"ctx": row + part * tiles, "dp": to_row},
            device_id_type=MESH,
        )

    for part in range(2):
        for o in range(1, ndp):
            copy_g2(part, lax.rem(row + o, ndp), me).start()
        mine = me == row + part * tiles

        @pl.when(mine)
        def _():
            g2_rx[me] = g2_send[part]

        @pl.when(jnp.logical_not(mine))
        def _():
            copy_g2(part, row, me).start()

    for peer in peers:
        copy_mg(peer, peer).wait_recv()

    from_row = lax.rem(me, tiles)
    for c in range(nctx):
        outside = jnp.logical_not(jnp.logical_and(me == c, row == from_row))

        @pl.when(outside)
        def _():
            copy_g2(0, row, c).wait_recv()

    for peer in peers:
        copy1(peer, me).wait_send()
        copyf(peer, me).wait_send()
        copy_mg(peer, me).wait_send()
    for peer in rows_peers:
        copy_rs(peer, row).wait_send()
    for part in range(2):
        for o in range(1, ndp):
            copy_g2(part, lax.rem(row + o, ndp), me).wait_send()

        @pl.when(jnp.logical_not(me == row + part * tiles))
        def _():
            copy_g2(part, row, me).wait_send()


def finish(mg, g2, q, k, v, g, out_hbm, gq_hbm, gk_hbm, gv_hbm, gf_hbm, out_v, gq_v, gk_v, gv_v, gf_v, sems):
    length = q.shape[1]
    hl = length // 2
    tiles = mg.shape[0] // 2
    low = lax.broadcasted_iota(jnp.int32, (length, LANES), 1) < LANES // 2
    low_h = lax.broadcasted_iota(jnp.int32, (hl, LANES), 1) < LANES // 2
    copies = []

    def put(n, p, src, dst):
        copy = pltpu.make_async_copy(src, dst, sems.at[n, p])
        copy.start()
        copies.append(copy)

    for p in range(tiles):
        cols = slice(p * LANES, (p + 1) * LANES)
        mixed, back = merge(mg[2 * p].astype(F32), mg[2 * p + 1].astype(F32), low)
        out_v[0, :, cols] = (q[0, :, cols].astype(F32) * mixed).astype(BF16)
        gq_v[0, :, cols] = (g[0, :, cols].astype(F32) * mixed).astype(BF16)
        gk_v[0, :, cols] = (v[0, :, cols].astype(F32) * back).astype(BF16)
        gv_v[0, :, cols] = (k[0, :, cols].astype(F32) * back).astype(BF16)
        top, bottom = merge(g2[2 * p].astype(F32), g2[2 * p + 1].astype(F32), low_h)
        gf_v[0:hl, cols] = top
        gf_v[hl:length, cols] = bottom
        for n, (src, dst) in enumerate(((out_v, out_hbm), (gq_v, gq_hbm), (gk_v, gk_hbm), (gv_v, gv_hbm))):
            put(n, p, src.at[:, :, cols], dst.at[:, :, cols])
        put(4, p, gf_v.at[:, cols], gf_hbm.at[:, cols])
    for copy in copies:
        copy.wait()


def fused(nctx, ndp, query, key_input, value_input, filter_taps, grad_output):
    length, channels = query.shape[1], query.shape[2]
    ahead, back = block_tables(length)
    vm = pl.BlockSpec(memory_space=pltpu.VMEM)
    hbm = pl.BlockSpec(memory_space=pltpu.HBM)
    hl, tiles = length // 2, nctx // 2
    dma = pltpu.SemaphoreType.DMA
    kept = 2 * (4 * query.size + nctx * (length + hl) * LANES) + 16384
    arrived = pl.pallas_call(
        functools.partial(kernel, nctx, ndp),
        out_shape=(
            pltpu.VMEM((nctx, length, LANES), BF16),
            pltpu.VMEM((nctx, hl, LANES), BF16),
            pltpu.VMEM(query.shape, BF16),
            pltpu.VMEM(query.shape, BF16),
            pltpu.VMEM(query.shape, BF16),
            pltpu.VMEM(query.shape, BF16),
        ),
        in_specs=[hbm] * 7,
        out_specs=(vm,) * 6,
        scratch_shapes=[
            pltpu.VMEM((length, channels), F32),
            pltpu.VMEM(ahead.shape, BF16),
            pltpu.VMEM(back.shape, BF16),
            pltpu.VMEM((nctx, length, LANES), BF16),
            pltpu.VMEM((nctx, length, LANES), BF16),
            pltpu.VMEM((nctx, hl, LANES), BF16),
            pltpu.VMEM((nctx, hl, LANES), BF16),
            pltpu.VMEM((nctx, 2 * length, LANES), F32),
            pltpu.VMEM((nctx, 2 * length, LANES), F32),
            pltpu.VMEM((nctx, 2 * length, LANES), F32),
            pltpu.VMEM((tiles, 2 * length, LANES), F32),
            pltpu.VMEM((tiles, length, LANES), BF16),
            pltpu.VMEM((ndp, length, LANES), BF16),
            pltpu.VMEM((2, hl, LANES), BF16),
            pltpu.VMEM((nctx, length, LANES), BF16),
            dma((7,)),
            dma((nctx,)),
            dma((nctx,)),
            dma((nctx,)),
            dma((nctx,)),
            dma((ndp,)),
            dma((ndp,)),
            dma((2, ndp)),
            dma((nctx,)),
            dma((nctx,)),
            dma((nctx,)),
        ],
        compiler_params=pltpu.CompilerParams(
            collective_id=0, has_side_effects=True, vmem_limit_bytes=VMEM_BYTES - kept
        ),
    )(query, key_input, value_input, filter_taps, grad_output, jnp.asarray(ahead), jnp.asarray(back))
    wide = jax.ShapeDtypeStruct(query.shape, BF16)
    return pl.pallas_call(
        finish,
        out_shape=(wide, wide, wide, wide, jax.ShapeDtypeStruct((length, channels), F32)),
        in_specs=[vm] * 6,
        out_specs=(hbm,) * 5,
        scratch_shapes=[pltpu.VMEM(query.shape, BF16)] * 4 + [pltpu.VMEM((length, channels), F32), dma((5, tiles))],
        compiler_params=pltpu.CompilerParams(vmem_limit_bytes=16 * 1024 * 1024),
    )(*arrived)


def build_tables(length):
    padded = 2 * length
    columns = 1
    while columns * columns < padded and length % (2 * columns) == 0:
        columns = columns * 2
    row_count = padded // columns
    col_index = jnp.arange(columns, dtype=jnp.int32)
    row_index = jnp.arange(row_count, dtype=jnp.int32)
    col_angle = (col_index[:, None] * col_index[None, :] % columns).astype(jnp.float32) * (
        2.0 * math.pi / columns
    )
    row_angle = (row_index[:, None] * row_index[None, :] % row_count).astype(jnp.float32) * (
        2.0 * math.pi / row_count
    )
    twist_angle = (row_index[:, None] * col_index[None, :] % padded).astype(jnp.float32) * (
        2.0 * math.pi / padded
    )
    return (
        jnp.cos(col_angle),
        -jnp.sin(col_angle),
        jnp.cos(row_angle),
        -jnp.sin(row_angle),
        jnp.cos(twist_angle),
        -jnp.sin(twist_angle),
        row_count,
        columns,
        padded,
    )


def forward(signal, tables):
    col_real, col_imag, row_real, row_imag, twist_real, twist_imag, row_count, columns, padded = (
        tables
    )
    half_rows = row_count // 2
    blocks = signal.reshape(signal.shape[0], half_rows, columns, signal.shape[2])
    section_real = jnp.einsum("kn,snac->scka", row_real[:, :half_rows], blocks, precision=HIGH)
    section_imag = jnp.einsum("kn,snac->scka", row_imag[:, :half_rows], blocks, precision=HIGH)
    turned_real = section_real * twist_real - section_imag * twist_imag
    turned_imag = section_real * twist_imag + section_imag * twist_real
    spec_real = jnp.einsum("scka,aj->sckj", turned_real, col_real, precision=HIGH) - jnp.einsum(
        "scka,aj->sckj", turned_imag, col_imag, precision=HIGH
    )
    spec_imag = jnp.einsum("scka,aj->sckj", turned_real, col_imag, precision=HIGH) + jnp.einsum(
        "scka,aj->sckj", turned_imag, col_real, precision=HIGH
    )
    return (spec_real, spec_imag)


def inverse(spec, tables):
    col_real, col_imag, row_real, row_imag, twist_real, twist_imag, row_count, columns, padded = (
        tables
    )
    spec_real, spec_imag = spec
    half_rows = row_count // 2
    section_real = jnp.einsum("scka,aj->sckj", spec_real, col_real, precision=HIGH) + jnp.einsum(
        "scka,aj->sckj", spec_imag, col_imag, precision=HIGH
    )
    section_imag = jnp.einsum("scka,aj->sckj", spec_imag, col_real, precision=HIGH) - jnp.einsum(
        "scka,aj->sckj", spec_real, col_imag, precision=HIGH
    )
    turned_real = section_real * twist_real + section_imag * twist_imag
    turned_imag = section_imag * twist_real - section_real * twist_imag
    signal = jnp.einsum(
        "nk,scka->snac", row_real[:half_rows], turned_real, precision=HIGH
    ) + jnp.einsum("nk,scka->snac", row_imag[:half_rows], turned_imag, precision=HIGH)
    return signal.reshape(signal.shape[0], half_rows * columns, signal.shape[3]) * (1.0 / padded)


def times_spec(first, second):
    return (
        first[0] * second[0] - first[1] * second[1],
        first[0] * second[1] + first[1] * second[0],
    )


def times_conj(first, second):
    return (
        first[0] * second[0] + first[1] * second[1],
        first[1] * second[0] - first[0] * second[1],
    )


def local(query, key_input, value_input, filter_taps, grad_output):
    product = (key_input.astype(jnp.float32) * value_input.astype(jnp.float32)).astype(jnp.bfloat16)
    grad_mix = (grad_output.astype(jnp.float32) * query.astype(jnp.float32)).astype(jnp.bfloat16)
    owned_filter = lax.all_to_all(filter_taps, "ctx", split_axis=1, concat_axis=0, tiled=True)
    tables = build_tables(owned_filter.shape[0])
    filter_spec = forward(owned_filter[None], tables)
    local_product = lax.all_to_all(product, "ctx", split_axis=2, concat_axis=1, tiled=True)
    prod_spec = forward(local_product.astype(jnp.float32), tables)
    owned_mixed = inverse(times_spec(filter_spec, prod_spec), tables).astype(jnp.bfloat16)
    owned_mixed, prod_spec = (owned_mixed, prod_spec)
    mixed = lax.all_to_all(owned_mixed, "ctx", split_axis=1, concat_axis=2, tiled=True)
    owned_grad = lax.all_to_all(grad_mix, "ctx", split_axis=2, concat_axis=1, tiled=True)
    grad_spec = forward(owned_grad.astype(jnp.float32), tables)
    owned_back = inverse(times_conj(grad_spec, filter_spec), tables).astype(jnp.bfloat16)
    taps_spec = times_conj(grad_spec, prod_spec)
    owned_back, taps_spec = (
        owned_back,
        (jnp.sum(taps_spec[0], axis=0), jnp.sum(taps_spec[1], axis=0)),
    )
    grad_product = lax.all_to_all(owned_back, "ctx", split_axis=1, concat_axis=2, tiled=True)
    mixed_wide = mixed.astype(jnp.float32)
    back_wide = grad_product.astype(jnp.float32)
    output = (query.astype(jnp.float32) * mixed_wide).astype(jnp.bfloat16)
    grad_query = (grad_output.astype(jnp.float32) * mixed_wide).astype(jnp.bfloat16)
    grad_key = (back_wide * value_input.astype(jnp.float32)).astype(jnp.bfloat16)
    grad_value = (back_wide * key_input.astype(jnp.float32)).astype(jnp.bfloat16)
    local_taps = inverse((taps_spec[0][None], taps_spec[1][None]), tables)[0]
    owned_taps = lax.psum(local_taps, "dp")
    grad_filter = lax.all_to_all(owned_taps, "ctx", split_axis=0, concat_axis=1, tiled=True)
    return (output, grad_query, grad_key, grad_value, grad_filter)


def plan(mesh, query, key_input, value_input, filter_taps, grad_output):
    nctx, ndp = mesh.shape["ctx"], mesh.shape["dp"]
    sequences, length, channels = query.shape
    fits = 2 * channels == nctx * LANES and nctx == 2 * ndp and sequences == 1 and length % 32 == 0 and length <= LANES
    run = functools.partial(fused, nctx, ndp) if fits else local
    return run(query, key_input, value_input, filter_taps, grad_output)


def solution(mesh):
    wide, taps = P("dp", "ctx", None), P("ctx", None)
    return jax.shard_map(
        functools.partial(plan, mesh),
        mesh=mesh,
        in_specs=(wide, wide, wide, taps, wide),
        out_specs=(wide, wide, wide, wide, taps),
        check_vma=False,
    )
```

```python
import functools
import math

import jax
import jax.numpy as jnp
import numpy as np
from jax import lax
from jax.experimental import pallas as pl
from jax.experimental.pallas import tpu as pltpu
from jax.sharding import PartitionSpec as P

HIGH = lax.Precision.HIGHEST
MESH = pl.DeviceIdType.MESH
LANES = 128
VMEM_BYTES = 67043328
F32 = jnp.float32
BF16 = jnp.bfloat16


def block_tables(length):
    odd = 2 * np.arange(length, dtype=np.int64)[:, None] + 1
    angle = (odd * np.arange(length, dtype=np.int64)[None, :] % (4 * length)) * (2.0 * math.pi / (4 * length))
    ahead = np.concatenate([np.cos(angle), -np.sin(angle)], axis=0).astype(np.float32)
    back = ahead.T / np.float32(length)

    def split(table):
        high = jnp.asarray(table).astype(BF16)
        low = (jnp.asarray(table) - high.astype(F32)).astype(BF16)
        return high, low

    with jax.ensure_compile_time_eval():
        ahead_high, ahead_low = split(ahead)
        back_high, back_low = split(back)
        return (
            np.asarray(jnp.concatenate([ahead_high, ahead_low], axis=1)),
            np.asarray(jnp.concatenate([back_high, back_low], axis=1)),
        )


def merge(first, second, low):
    half = first.shape[-1] // 2
    turned = pltpu.roll(jnp.where(low, second, first), half, 1)
    return jnp.where(low, first, turned), jnp.where(low, turned, second)


def kernel(
    nctx,
    ndp,
    q_hbm,
    k_hbm,
    v_hbm,
    f_hbm,
    g_hbm,
    ahead_hbm,
    back_hbm,
    mg_rx,
    g2_rx,
    qv,
    kv,
    vv,
    gv,
    fv,
    ahead_v,
    back_v,
    send1,
    rx1,
    sendf,
    rxf,
    sig,
    wei,
    oth,
    gfs,
    rs_send,
    rs_rx,
    g2_send,
    mg_send,
    known,
    load_sem,
    s1_send,
    s1_recv,
    sf_send,
    sf_recv,
    rs_ssem,
    rs_rsem,
    g2_ssem,
    g2_rsem,
    mg_ssem,
    mg_rsem,
):
    me = lax.axis_index("ctx")
    row = lax.axis_index("dp")
    length = qv.shape[1]
    hl = length // 2
    tiles = nctx // 2

    pairs = ((k_hbm, kv), (v_hbm, vv), (g_hbm, gv), (q_hbm, qv), (f_hbm, fv), (ahead_hbm, ahead_v), (back_hbm, back_v))
    loads = [pltpu.make_async_copy(src, dst, load_sem.at[n]) for n, (src, dst) in enumerate(pairs)]
    for load in loads:
        load.start()

    barrier = pltpu.get_barrier_semaphore()
    for oc in range(1, nctx):
        pl.semaphore_signal(
            barrier, inc=1, device_id={"ctx": lax.rem(me + oc, nctx), "dp": row}, device_id_type=MESH
        )
    for step, there in ((1, row + 1 < ndp), (-1, row > 0)):

        @pl.when(there)
        def _(step=step):
            pl.semaphore_signal(barrier, inc=1, device_id={"ctx": me, "dp": row + step}, device_id_type=MESH)

    low = lax.broadcasted_iota(jnp.int32, (length, LANES), 1) < LANES // 2
    low_h = lax.broadcasted_iota(jnp.int32, (hl, LANES), 1) < LANES // 2
    for load in loads[:4]:
        load.wait()
    for p in range(tiles):
        cols = slice(p * LANES, (p + 1) * LANES)
        x = (kv[0, :, cols].astype(F32) * vv[0, :, cols].astype(F32)).astype(BF16).astype(F32)
        g = (gv[0, :, cols].astype(F32) * qv[0, :, cols].astype(F32)).astype(BF16).astype(F32)
        even, odd = merge(x, g, low)
        send1[2 * p] = even.astype(BF16)
        send1[2 * p + 1] = odd.astype(BF16)

    beside = jnp.where(row + 1 < ndp, 1, 0) + jnp.where(row > 0, 1, 0)
    pl.semaphore_wait(barrier, nctx - 1 + beside)

    def copy1(peer, slot):
        return pltpu.make_async_remote_copy(
            src_ref=send1.at[peer],
            dst_ref=rx1.at[slot],
            send_sem=s1_send.at[peer],
            recv_sem=s1_recv.at[slot],
            device_id={"ctx": peer, "dp": row},
            device_id_type=MESH,
        )

    def copyf(peer, slot):
        return pltpu.make_async_remote_copy(
            src_ref=sendf.at[peer],
            dst_ref=rxf.at[slot],
            send_sem=sf_send.at[peer],
            recv_sem=sf_recv.at[slot],
            device_id={"ctx": peer, "dp": row},
            device_id_type=MESH,
        )

    order = [nctx // 2 + o for o in range(nctx // 2)] + list(range(1, nctx // 2))
    peers = [lax.rem(me + o, nctx) for o in order]
    for peer in peers:
        copy1(peer, me).start()
    for n, (step, dist) in enumerate(((1, row), (-1, ndp - 1 - row))):

        @pl.when(dist >= 2)
        def _(n=n):
            pl.semaphore_wait(known.at[n], 1)

        @pl.when(jnp.logical_and(dist >= 1, dist + 1 < ndp))
        def _(n=n, step=step):
            pl.semaphore_signal(
                known.at[n], inc=1, device_id={"ctx": me, "dp": row + step}, device_id_type=MESH
            )

    loads[4].wait()
    for p in range(tiles):
        cols = slice(p * LANES, (p + 1) * LANES)
        even, odd = merge(fv[0:hl, cols], fv[hl:length, cols], low_h)
        sendf[2 * p] = even.astype(BF16)
        sendf[2 * p + 1] = odd.astype(BF16)
    for load in loads[5:]:
        load.wait()
    for peer in peers:
        copyf(peer, me).start()

    def transform(z):
        return jnp.dot(ahead_v[...], jnp.concatenate([z, z], axis=0), preferred_element_type=F32)

    def weigh(fa):
        fa = fa.astype(F32)
        turned = pltpu.roll(fa, LANES // 2, 1)
        w = jnp.concatenate([jnp.where(low_h, fa, turned), jnp.where(low_h, turned, fa)], axis=0)
        return transform(w.astype(BF16))

    sig[me] = transform(send1[me])
    for peer in reversed(peers):
        copy1(peer, peer).wait_recv()
        sig[peer] = transform(rx1[peer])

    lane8 = lax.broadcasted_iota(jnp.int32, (8, LANES), 1) < LANES // 2
    parity = lax.rem(lax.broadcasted_iota(jnp.int32, (8, LANES), 0), 2)
    alt = jnp.where(parity == 0, 1.0, -1.0).astype(F32)
    lane_sign = jnp.where(lane8, 1.0, -1.0).astype(F32)
    both_sign = alt * lane_sign

    @pl.loop(0, length // 8)
    def _(i):
        re = pl.ds(pl.multiple_of(i * 8, 8), 8)
        im = pl.ds(pl.multiple_of(length + i * 8, 8), 8)
        s_re = [sig[d, re, :] for d in range(nctx)]
        s_im = [sig[d, im, :] for d in range(nctx)]
        u_re = [jnp.where(lane8, pltpu.roll(a, LANES // 2, 1), a) for a in s_re]
        u_im = [jnp.where(lane8, pltpu.roll(a, LANES // 2, 1), a) for a in s_im]
        x_re = [s_re[0]] + [s_re[n] - alt * s_im[n - 1] for n in range(1, nctx)]
        x_im = [s_im[0]] + [s_im[n] + alt * s_re[n - 1] for n in range(1, nctx)]
        v_re = [jnp.where(lane8, x_re[n], 0.0) for n in range(tiles)]
        v_im = [jnp.where(lane8, x_im[n], 0.0) for n in range(tiles)]
        for n in range(tiles, nctx):
            v_re.append(jnp.where(lane8, x_re[n], pltpu.roll(x_re[n - tiles], LANES // 2, 1)))
            v_im.append(jnp.where(lane8, x_im[n], pltpu.roll(x_im[n - tiles], LANES // 2, 1)))
        for j in range(tiles):
            a_re = jnp.zeros((8, LANES), F32)
            a_im = jnp.zeros((8, LANES), F32)
            for m in range(j, nctx):
                n = m - j
                a_re = a_re + u_re[m] * v_re[n] + u_im[m] * v_im[n]
                a_im = a_im + u_im[m] * v_re[n] - u_re[m] * v_im[n]
            gfs[j, re, :] = a_re
            gfs[j, im, :] = a_im

    def inverse(spec):
        high = spec.astype(BF16)
        return jnp.dot(back_v[...], jnp.concatenate([high, high], axis=0), preferred_element_type=F32)

    def copy_rs(peer, slot):
        return pltpu.make_async_remote_copy(
            src_ref=rs_send.at[peer],
            dst_ref=rs_rx.at[slot],
            send_sem=rs_ssem.at[peer],
            recv_sem=rs_rsem.at[slot],
            device_id={"ctx": me, "dp": peer},
            device_id_type=MESH,
        )

    for j in range(tiles):
        rs_send[j] = inverse(gfs[j]).astype(BF16)
    rows_peers = [lax.rem(row + o, ndp) for o in range(1, ndp)]
    for peer in rows_peers:
        copy_rs(peer, row).start()

    wei[me] = weigh(sendf[me])
    for peer in reversed(peers):
        copyf(peer, peer).wait_recv()
        wei[peer] = weigh(rxf[peer])

    @pl.loop(0, length // 8)
    def _(i):
        re = pl.ds(pl.multiple_of(i * 8, 8), 8)
        im = pl.ds(pl.multiple_of(length + i * 8, 8), 8)
        s_re = [sig[d, re, :] for d in range(nctx)]
        s_im = [sig[d, im, :] for d in range(nctx)]
        q_re = [jnp.where(lane8, s_re[n], s_re[nctx - 1 - n]) for n in range(nctx)]
        q_im = [jnp.where(lane8, s_im[n], s_im[nctx - 1 - n]) for n in range(nctx)]
        z_re = [q_re[0]] + [q_re[n] - both_sign * q_im[n - 1] for n in range(1, nctx)]
        z_im = [q_im[0]] + [q_im[n] + both_sign * q_re[n - 1] for n in range(1, nctx)]
        w_re = [wei[d, re, :] for d in range(nctx)]
        w_im = [wei[d, im, :] * lane_sign for d in range(nctx)]
        o_re, o_im = [], []
        for n in range(nctx):
            a_re = jnp.zeros((8, LANES), F32)
            a_im = jnp.zeros((8, LANES), F32)
            for j in range(n + 1):
                a_re = a_re + w_re[j] * z_re[n - j] - w_im[j] * z_im[n - j]
                a_im = a_im + w_re[j] * z_im[n - j] + w_im[j] * z_re[n - j]
            o_re.append(a_re)
            o_im.append(a_im)
        for d in range(nctx):
            oth[d, re, :] = jnp.where(lane8, o_re[d], o_re[nctx - 1 - d])
            oth[d, im, :] = jnp.where(lane8, o_im[d], o_im[nctx - 1 - d])

    def copy_mg(peer, slot):
        return pltpu.make_async_remote_copy(
            src_ref=mg_send.at[peer],
            dst_ref=mg_rx.at[slot],
            send_sem=mg_ssem.at[peer],
            recv_sem=mg_rsem.at[slot],
            device_id={"ctx": peer, "dp": row},
            device_id_type=MESH,
        )

    for at, peer in enumerate(peers):
        mg_send[peer] = inverse(oth[peer]).astype(BF16)
        if at:
            copy_mg(peers[at - 1], me).start()
    mg_rx[me] = inverse(oth[me]).astype(BF16)
    copy_mg(peers[-1], me).start()

    total = rs_send[row].astype(F32)
    for peer in rows_peers:
        copy_rs(peer, peer).wait_recv()
        total = total + rs_rx[peer].astype(F32)
    first, second = merge(total[0:hl], total[hl:length], low_h)
    g2_send[0] = first.astype(BF16)
    g2_send[1] = second.astype(BF16)

    def copy_g2(part, to_row, slot):
        return pltpu.make_async_remote_copy(
            src_ref=g2_send.at[part],
            dst_ref=g2_rx.at[slot],
            send_sem=g2_ssem.at[part, to_row],
            recv_sem=g2_rsem.at[slot],
            device_id={"ctx": row + part * tiles, "dp": to_row},
            device_id_type=MESH,
        )

    for part in range(2):
        for o in range(1, ndp):
            copy_g2(part, lax.rem(row + o, ndp), me).start()
        mine = me == row + part * tiles

        @pl.when(mine)
        def _():
            g2_rx[me] = g2_send[part]

        @pl.when(jnp.logical_not(mine))
        def _():
            copy_g2(part, row, me).start()

    for peer in peers:
        copy_mg(peer, peer).wait_recv()

    from_row = lax.rem(me, tiles)
    for c in range(nctx):
        outside = jnp.logical_not(jnp.logical_and(me == c, row == from_row))

        @pl.when(outside)
        def _():
            copy_g2(0, row, c).wait_recv()

    for peer in peers:
        copy1(peer, me).wait_send()
        copyf(peer, me).wait_send()
        copy_mg(peer, me).wait_send()
    for peer in rows_peers:
        copy_rs(peer, row).wait_send()
    for part in range(2):
        for o in range(1, ndp):
            copy_g2(part, lax.rem(row + o, ndp), me).wait_send()

        @pl.when(jnp.logical_not(me == row + part * tiles))
        def _():
            copy_g2(part, row, me).wait_send()


def finish(mg, g2, q, k, v, g, out_hbm, gq_hbm, gk_hbm, gv_hbm, gf_hbm, out_v, gq_v, gk_v, gv_v, gf_v, sems):
    length = q.shape[1]
    hl = length // 2
    tiles = mg.shape[0] // 2
    low = lax.broadcasted_iota(jnp.int32, (length, LANES), 1) < LANES // 2
    low_h = lax.broadcasted_iota(jnp.int32, (hl, LANES), 1) < LANES // 2
    copies = []

    def put(n, p, src, dst):
        copy = pltpu.make_async_copy(src, dst, sems.at[n, p])
        copy.start()
        copies.append(copy)

    for p in range(tiles):
        cols = slice(p * LANES, (p + 1) * LANES)
        mixed, back = merge(mg[2 * p].astype(F32), mg[2 * p + 1].astype(F32), low)
        out_v[0, :, cols] = (q[0, :, cols].astype(F32) * mixed).astype(BF16)
        gq_v[0, :, cols] = (g[0, :, cols].astype(F32) * mixed).astype(BF16)
        gk_v[0, :, cols] = (v[0, :, cols].astype(F32) * back).astype(BF16)
        gv_v[0, :, cols] = (k[0, :, cols].astype(F32) * back).astype(BF16)
        top, bottom = merge(g2[2 * p].astype(F32), g2[2 * p + 1].astype(F32), low_h)
        gf_v[0:hl, cols] = top
        gf_v[hl:length, cols] = bottom
        for n, (src, dst) in enumerate(((out_v, out_hbm), (gq_v, gq_hbm), (gk_v, gk_hbm), (gv_v, gv_hbm))):
            put(n, p, src.at[:, :, cols], dst.at[:, :, cols])
        put(4, p, gf_v.at[:, cols], gf_hbm.at[:, cols])
    for copy in copies:
        copy.wait()


def fused(nctx, ndp, query, key_input, value_input, filter_taps, grad_output):
    length, channels = query.shape[1], query.shape[2]
    ahead, back = block_tables(length)
    vm = pl.BlockSpec(memory_space=pltpu.VMEM)
    hbm = pl.BlockSpec(memory_space=pltpu.HBM)
    hl, tiles = length // 2, nctx // 2
    dma = pltpu.SemaphoreType.DMA
    kept = 2 * (4 * query.size + nctx * (length + hl) * LANES) + 16384
    arrived = pl.pallas_call(
        functools.partial(kernel, nctx, ndp),
        out_shape=(
            pltpu.VMEM((nctx, length, LANES), BF16),
            pltpu.VMEM((nctx, hl, LANES), BF16),
            pltpu.VMEM(query.shape, BF16),
            pltpu.VMEM(query.shape, BF16),
            pltpu.VMEM(query.shape, BF16),
            pltpu.VMEM(query.shape, BF16),
        ),
        in_specs=[hbm] * 7,
        out_specs=(vm,) * 6,
        scratch_shapes=[
            pltpu.VMEM((length, channels), F32),
            pltpu.VMEM(ahead.shape, BF16),
            pltpu.VMEM(back.shape, BF16),
            pltpu.VMEM((nctx, length, LANES), BF16),
            pltpu.VMEM((nctx, length, LANES), BF16),
            pltpu.VMEM((nctx, hl, LANES), BF16),
            pltpu.VMEM((nctx, hl, LANES), BF16),
            pltpu.VMEM((nctx, 2 * length, LANES), F32),
            pltpu.VMEM((nctx, 2 * length, LANES), F32),
            pltpu.VMEM((nctx, 2 * length, LANES), F32),
            pltpu.VMEM((tiles, 2 * length, LANES), F32),
            pltpu.VMEM((tiles, length, LANES), BF16),
            pltpu.VMEM((ndp, length, LANES), BF16),
            pltpu.VMEM((2, hl, LANES), BF16),
            pltpu.VMEM((nctx, length, LANES), BF16),
            pltpu.SemaphoreType.REGULAR((2,)),
            dma((7,)),
            dma((nctx,)),
            dma((nctx,)),
            dma((nctx,)),
            dma((nctx,)),
            dma((ndp,)),
            dma((ndp,)),
            dma((2, ndp)),
            dma((nctx,)),
            dma((nctx,)),
            dma((nctx,)),
        ],
        compiler_params=pltpu.CompilerParams(
            collective_id=0, has_side_effects=True, vmem_limit_bytes=VMEM_BYTES - kept
        ),
    )(query, key_input, value_input, filter_taps, grad_output, jnp.asarray(ahead), jnp.asarray(back))
    wide = jax.ShapeDtypeStruct(query.shape, BF16)
    return pl.pallas_call(
        finish,
        out_shape=(wide, wide, wide, wide, jax.ShapeDtypeStruct((length, channels), F32)),
        in_specs=[vm] * 6,
        out_specs=(hbm,) * 5,
        scratch_shapes=[pltpu.VMEM(query.shape, BF16)] * 4 + [pltpu.VMEM((length, channels), F32), dma((5, tiles))],
        compiler_params=pltpu.CompilerParams(vmem_limit_bytes=16 * 1024 * 1024),
    )(*arrived)


def build_tables(length):
    padded = 2 * length
    columns = 1
    while columns * columns < padded and length % (2 * columns) == 0:
        columns = columns * 2
    row_count = padded // columns
    col_index = jnp.arange(columns, dtype=jnp.int32)
    row_index = jnp.arange(row_count, dtype=jnp.int32)
    col_angle = (col_index[:, None] * col_index[None, :] % columns).astype(jnp.float32) * (
        2.0 * math.pi / columns
    )
    row_angle = (row_index[:, None] * row_index[None, :] % row_count).astype(jnp.float32) * (
        2.0 * math.pi / row_count
    )
    twist_angle = (row_index[:, None] * col_index[None, :] % padded).astype(jnp.float32) * (
        2.0 * math.pi / padded
    )
    return (
        jnp.cos(col_angle),
        -jnp.sin(col_angle),
        jnp.cos(row_angle),
        -jnp.sin(row_angle),
        jnp.cos(twist_angle),
        -jnp.sin(twist_angle),
        row_count,
        columns,
        padded,
    )


def forward(signal, tables):
    col_real, col_imag, row_real, row_imag, twist_real, twist_imag, row_count, columns, padded = (
        tables
    )
    half_rows = row_count // 2
    blocks = signal.reshape(signal.shape[0], half_rows, columns, signal.shape[2])
    section_real = jnp.einsum("kn,snac->scka", row_real[:, :half_rows], blocks, precision=HIGH)
    section_imag = jnp.einsum("kn,snac->scka", row_imag[:, :half_rows], blocks, precision=HIGH)
    turned_real = section_real * twist_real - section_imag * twist_imag
    turned_imag = section_real * twist_imag + section_imag * twist_real
    spec_real = jnp.einsum("scka,aj->sckj", turned_real, col_real, precision=HIGH) - jnp.einsum(
        "scka,aj->sckj", turned_imag, col_imag, precision=HIGH
    )
    spec_imag = jnp.einsum("scka,aj->sckj", turned_real, col_imag, precision=HIGH) + jnp.einsum(
        "scka,aj->sckj", turned_imag, col_real, precision=HIGH
    )
    return (spec_real, spec_imag)


def inverse(spec, tables):
    col_real, col_imag, row_real, row_imag, twist_real, twist_imag, row_count, columns, padded = (
        tables
    )
    spec_real, spec_imag = spec
    half_rows = row_count // 2
    section_real = jnp.einsum("scka,aj->sckj", spec_real, col_real, precision=HIGH) + jnp.einsum(
        "scka,aj->sckj", spec_imag, col_imag, precision=HIGH
    )
    section_imag = jnp.einsum("scka,aj->sckj", spec_imag, col_real, precision=HIGH) - jnp.einsum(
        "scka,aj->sckj", spec_real, col_imag, precision=HIGH
    )
    turned_real = section_real * twist_real + section_imag * twist_imag
    turned_imag = section_imag * twist_real - section_real * twist_imag
    signal = jnp.einsum(
        "nk,scka->snac", row_real[:half_rows], turned_real, precision=HIGH
    ) + jnp.einsum("nk,scka->snac", row_imag[:half_rows], turned_imag, precision=HIGH)
    return signal.reshape(signal.shape[0], half_rows * columns, signal.shape[3]) * (1.0 / padded)


def times_spec(first, second):
    return (
        first[0] * second[0] - first[1] * second[1],
        first[0] * second[1] + first[1] * second[0],
    )


def times_conj(first, second):
    return (
        first[0] * second[0] + first[1] * second[1],
        first[1] * second[0] - first[0] * second[1],
    )


def local(query, key_input, value_input, filter_taps, grad_output):
    product = (key_input.astype(jnp.float32) * value_input.astype(jnp.float32)).astype(jnp.bfloat16)
    grad_mix = (grad_output.astype(jnp.float32) * query.astype(jnp.float32)).astype(jnp.bfloat16)
    owned_filter = lax.all_to_all(filter_taps, "ctx", split_axis=1, concat_axis=0, tiled=True)
    tables = build_tables(owned_filter.shape[0])
    filter_spec = forward(owned_filter[None], tables)
    local_product = lax.all_to_all(product, "ctx", split_axis=2, concat_axis=1, tiled=True)
    prod_spec = forward(local_product.astype(jnp.float32), tables)
    owned_mixed = inverse(times_spec(filter_spec, prod_spec), tables).astype(jnp.bfloat16)
    owned_mixed, prod_spec = (owned_mixed, prod_spec)
    mixed = lax.all_to_all(owned_mixed, "ctx", split_axis=1, concat_axis=2, tiled=True)
    owned_grad = lax.all_to_all(grad_mix, "ctx", split_axis=2, concat_axis=1, tiled=True)
    grad_spec = forward(owned_grad.astype(jnp.float32), tables)
    owned_back = inverse(times_conj(grad_spec, filter_spec), tables).astype(jnp.bfloat16)
    taps_spec = times_conj(grad_spec, prod_spec)
    owned_back, taps_spec = (
        owned_back,
        (jnp.sum(taps_spec[0], axis=0), jnp.sum(taps_spec[1], axis=0)),
    )
    grad_product = lax.all_to_all(owned_back, "ctx", split_axis=1, concat_axis=2, tiled=True)
    mixed_wide = mixed.astype(jnp.float32)
    back_wide = grad_product.astype(jnp.float32)
    output = (query.astype(jnp.float32) * mixed_wide).astype(jnp.bfloat16)
    grad_query = (grad_output.astype(jnp.float32) * mixed_wide).astype(jnp.bfloat16)
    grad_key = (back_wide * value_input.astype(jnp.float32)).astype(jnp.bfloat16)
    grad_value = (back_wide * key_input.astype(jnp.float32)).astype(jnp.bfloat16)
    local_taps = inverse((taps_spec[0][None], taps_spec[1][None]), tables)[0]
    owned_taps = lax.psum(local_taps, "dp")
    grad_filter = lax.all_to_all(owned_taps, "ctx", split_axis=0, concat_axis=1, tiled=True)
    return (output, grad_query, grad_key, grad_value, grad_filter)


def plan(mesh, query, key_input, value_input, filter_taps, grad_output):
    nctx, ndp = mesh.shape["ctx"], mesh.shape["dp"]
    sequences, length, channels = query.shape
    fits = 2 * channels == nctx * LANES and nctx == 2 * ndp and sequences == 1 and length % 32 == 0 and length <= LANES
    run = functools.partial(fused, nctx, ndp) if fits else local
    return run(query, key_input, value_input, filter_taps, grad_output)


def solution(mesh):
    wide, taps = P("dp", "ctx", None), P("ctx", None)
    return jax.shard_map(
        functools.partial(plan, mesh),
        mesh=mesh,
        in_specs=(wide, wide, wide, taps, wide),
        out_specs=(wide, wide, wide, wide, taps),
        check_vma=False,
    )
```
